32 devices in a mesh: wide: 16 (over z, y, x), narrow: 2 (over core).
Axes of the slice: x: 2, y: 2, z: 4, core: 2. Of those that a mesh axis runs over, the one named last changes fastest.
Arguments:
- contributions: float32 [2, 3, 8192, 128], P('narrow', None, 'wide'), may hold values from -6 to 6
- send_map: int32 [16, 800], P('wide'), may hold values from -1 to 511, as said below
- arrival_map: int32 [16, 800], P('wide'), may hold values from -1 to 255, as said below
- dual_diagonal: float32 [4096, 128], P('wide'), may hold values from 0.5 to 2
- mortar: bfloat16 [4096, 128, 128], P('wide'), may hold values from -0.5 to 0.5
- master_inverse: bfloat16 [4096, 128, 128], P('wide'), may hold values from -0.5 to 0.5
Outputs:
- corrections: float32 [2, 3, 8192, 128], P('narrow', None, 'wide')
The draws below stay inside these ranges and needn't reach their ends.
Inputs may be any that keep to these rules, and one draw needn't show every extreme that they name: `send_map`: each row 0 to 511 of a partition stands in exactly one of its slots. Some stripe has all 50 of its slots used by every partition. arrival_map[d, o * 50 + c] is -1 exactly where send_map[o, d * 50 + c] is -1.
All inputs are finite; a program needn't handle non-finite values.
Results may differ from the reference program's by a relative error of at most 0.0041.
Values sent between devices are 32-bit elements; how exact they have to be, the bound alone decides.
A program may use at most 64 MiB of HBM per device.

```python
import math
import jax
import jax.numpy as jnp
from jax import lax

NODES = 128
COMP = 3
BLK_DEV = 256
BLOCKS = 4096
ROWS_OWN = 512
ROWS = 8192
CAP = 50
SLOTS = 800
N_WIDE = 16


def shared_maps(key):
    base = jax.random.fold_in(key, 7)
    key_hot, key_bias, key_jitter, key_tie, key_rows, key_block = jax.random.split(base, 6)
    hot_stripe = jax.random.randint(key_hot, (), 0, N_WIDE)
    stripe_bias = jax.random.randint(key_bias, (N_WIDE,), 0, 4)
    stripe_bias = stripe_bias * stripe_bias
    stripe_ids = jnp.arange(SLOTS, dtype=jnp.int32) // CAP
    random_perturbation = jax.random.randint(key_jitter, (N_WIDE, SLOTS), 0, 16)
    scores = jnp.where(stripe_ids[None, :] == hot_stripe, 1000, stripe_bias[stripe_ids][None, :] + random_perturbation)
    raw_ties = jax.random.randint(key_tie, (N_WIDE, SLOTS), 0, 1 << 30)
    tie_rank = jnp.argsort(jnp.argsort(raw_ties, axis=1), axis=1)
    priority_order = jnp.argsort(-(scores * SLOTS + tie_rank), axis=1)
    chosen = priority_order[:, :ROWS_OWN]
    row_order = jnp.argsort(jax.random.randint(key_rows, (N_WIDE, ROWS_OWN), 0, 1 << 30), axis=1).astype(jnp.int32)
    owners = jnp.arange(N_WIDE, dtype=jnp.int32)[:, None]
    send_map = jnp.full((N_WIDE, SLOTS), -1, jnp.int32).at[owners, chosen].set(row_order)
    by_stripe = jnp.transpose(send_map.reshape(N_WIDE, N_WIDE, CAP), (1, 0, 2)).reshape(N_WIDE, SLOTS)
    local_ids = jax.random.randint(key_block, (N_WIDE, SLOTS), 0, BLK_DEV)
    arrival_map = jnp.where(by_stripe >= 0, local_ids, -1).astype(jnp.int32)
    return (send_map, arrival_map)


def draw_send_map(key, part):
    return shared_maps(key)[0]


def draw_arrival_map(key, part):
    return shared_maps(key)[1]


def steps_of(key, shape, cuts, least, largest):
    def one(axis_at, shards_of):
        steps = jax.random.uniform(jax.random.fold_in(jax.random.fold_in(key, 6), axis_at), (shards_of,), jnp.float32, least / len(cuts), largest / len(cuts))
        return jnp.repeat(jnp.exp(steps), shape[axis_at] // shards_of).reshape((-1,) + (1,) * (len(shape) - axis_at - 1))

    level = one(*cuts[0])
    for cut in cuts[1:]:
        level = level * one(*cut)
    return level


def bell_draw(rng, shape, scale, most, cuts=(), kind=jnp.bfloat16):
    drawn = scale * jax.random.normal(rng, shape, jnp.float32)
    if cuts:
        drawn = drawn * steps_of(rng, shape, cuts, -0.22, 0.18)
    return jnp.clip(drawn, -most, most).astype(kind)


def setup_inputs(seed: int = 0) -> dict:
    seeds = jax.random.split(jax.random.key(seed), 7)
    return {
        "contributions": bell_draw(seeds[0], (2, COMP, ROWS, NODES), 1.0, 6.0, ((0, 2), (2, 16)), jnp.float32),
        "send_map": draw_send_map(jax.random.fold_in(seeds[6], 71), 0),
        "arrival_map": draw_arrival_map(jax.random.fold_in(seeds[6], 71), 0),
        "dual_diagonal": jnp.clip(jnp.exp(math.log(2.0) - 1.3862944 * jax.random.uniform(seeds[3], (BLOCKS, NODES), jnp.float32) ** steps_of(seeds[3], (BLOCKS, NODES), ((0, 16),), -0.2, 0.2)), 0.5, 2.0),
        "mortar": bell_draw(seeds[4], (BLOCKS, NODES, NODES), NODES ** -0.5, 0.5, ((0, 16),)),
        "master_inverse": bell_draw(seeds[5], (BLOCKS, NODES, NODES), NODES ** -0.5, 0.5, ((0, 16),)),
    }


def stripe_solve(pieces):
    summed, diagonal, mortar_part, inverse_part = pieces
    mortar_wide = mortar_part.astype(jnp.float32)
    inverse_wide = inverse_part.astype(jnp.float32)
    multiplier = summed[0] / diagonal[None]
    multiplier_low = lax.optimization_barrier(multiplier.astype(jnp.bfloat16)).astype(jnp.float32)
    pushed = jnp.einsum('bij,cbi->cbj', mortar_wide, multiplier_low, precision=lax.Precision.HIGHEST)
    condensed = summed[1] + pushed
    condensed_low = lax.optimization_barrier(condensed.astype(jnp.bfloat16)).astype(jnp.float32)
    master_fix = jnp.einsum('bkj,cbj->cbk', inverse_wide, condensed_low, precision=lax.Precision.HIGHEST)
    master_low = lax.optimization_barrier(master_fix.astype(jnp.bfloat16)).astype(jnp.float32)
    slave_fix = jnp.einsum('bij,cbj->cbi', mortar_wide, master_low, precision=lax.Precision.HIGHEST) / diagonal[None]
    return jnp.stack([slave_fix, master_fix])


def reference(contributions, send_map, arrival_map, dual_diagonal, mortar, master_inverse):
    owners = jnp.arange(N_WIDE, dtype=jnp.int32)[:, None]
    slot_ids = jnp.arange(SLOTS, dtype=jnp.int32)[None, :]
    stripes = slot_ids // CAP
    local_block = arrival_map[stripes, owners * CAP + slot_ids % CAP]
    is_live = send_map >= 0
    targets = jnp.where(is_live, owners * ROWS_OWN + send_map, ROWS).astype(jnp.int32)
    block_ids = (stripes * BLK_DEV + local_block).astype(jnp.int32)
    row_block = jnp.zeros((ROWS + 1,), jnp.int32).at[targets.reshape(-1)].set(block_ids.reshape(-1))[:ROWS]
    summed = jnp.zeros((2, COMP, BLOCKS, NODES), jnp.float32).at[:, :, row_block, :].add(contributions)
    by_stripe = jnp.transpose(summed.reshape(2, COMP, N_WIDE, BLK_DEV, NODES), (2, 0, 1, 3, 4))
    diag_parts = dual_diagonal.reshape(N_WIDE, BLK_DEV, NODES)
    mortar_parts = mortar.reshape(N_WIDE, BLK_DEV, NODES, NODES)
    inverse_parts = master_inverse.reshape(N_WIDE, BLK_DEV, NODES, NODES)
    fixes = lax.map(stripe_solve, (by_stripe, diag_parts, mortar_parts, inverse_parts))
    fixes = jnp.transpose(fixes, (1, 2, 0, 3, 4)).reshape(2, COMP, BLOCKS, NODES)
    return fixes[:, :, row_block, :]
```

```python
import functools

import jax
import jax.numpy as jnp
from jax import lax
from jax.experimental import pallas as pl
from jax.experimental.pallas import tpu as pltpu
from jax.sharding import PartitionSpec as P

GROUP = 16
SUBLANES = 8


def one_hot_dot(mask, values):
    high = values.astype(jnp.bfloat16)
    low = (values - high.astype(jnp.float32)).astype(jnp.bfloat16)
    return jnp.dot(mask, high, preferred_element_type=jnp.float32) + jnp.dot(
        mask, low, preferred_element_type=jnp.float32
    )


def block_products(vectors, matrices, transposed):
    rows = lax.broadcasted_iota(jnp.int32, vectors.shape, 0)
    total = jnp.zeros(vectors.shape, jnp.float32)
    for b in range(vectors.shape[0]):
        product = lax.dot_general(
            vectors,
            matrices(b),
            (((1,), (1 if transposed else 0,)), ((), ())),
            preferred_element_type=jnp.float32,
        )
        total = jnp.where(rows == b, product, total)
    return total


def kernel(
    n,
    cap,
    contributions,
    send_col,
    send_row,
    arrival_col,
    arrival_row,
    diagonal,
    mortar_hbm,
    inverse_hbm,
    out,
    pick_mask,
    sum_mask,
    spread_mask,
    place_mask,
    going,
    coming,
    returning,
    returned,
    sums,
    other_sums,
    other_fix,
    fixes,
    mortar,
    inverse,
    fetch_sem,
    wide_send,
    wide_recv,
    pair_send,
    pair_recv,
):
    me = lax.axis_index("wide")
    side = lax.axis_index("narrow")
    comps, row_count, nodes = out.shape[1:]
    capp = coming.shape[2]
    slots = n * capp
    half = mortar.shape[0]

    fetches = [
        pltpu.make_async_copy(mortar_hbm.at[pl.ds(side * half, half)], mortar, fetch_sem.at[0]),
        pltpu.make_async_copy(inverse_hbm.at[pl.ds(side * half, half)], inverse, fetch_sem.at[1]),
    ]

    if capp > cap:
        last = pl.ds(capp - SUBLANES, SUBLANES)
        empty = jnp.zeros((comps, n, SUBLANES, nodes), jnp.float32)
        coming[:, :, last, :] = empty
        returned[:, :, last, :] = empty

    barrier = pltpu.get_barrier_semaphore()

    def greet(k, carry):
        pl.semaphore_signal(barrier, inc=1, device_id={"wide": lax.rem(me + k, n)}, device_id_type=pl.DeviceIdType.MESH)
        return carry

    lax.fori_loop(1, n, greet, 0)
    pl.semaphore_signal(barrier, inc=1, device_id={"narrow": 1 - side}, device_id_type=pl.DeviceIdType.MESH)
    for fetch in fetches:
        fetch.start()


    def mask_of(ids, shape, axis):
        return jnp.where(ids == lax.broadcasted_iota(jnp.int32, shape, axis), 1.0, 0.0).astype(jnp.bfloat16)

    def row_mask_of(ids, shape):
        tiles = (shape[0] // SUBLANES, SUBLANES, shape[1])
        rows = lax.broadcasted_iota(jnp.int32, tiles, 0) * SUBLANES + lax.broadcasted_iota(
            jnp.int32, tiles, 1
        )
        return jnp.where(ids[None] == rows, 1.0, 0.0).reshape(shape).astype(jnp.bfloat16)

    pick_mask[...] = mask_of(send_col[...], pick_mask.shape, 1)

    def exchange(source, target, c, phase):
        def one_copy(peer):
            pltpu.make_async_remote_copy(
                src_ref=source.at[c, peer, pl.ds(0, cap)],
                dst_ref=target.at[c, me, pl.ds(0, cap)],
                send_sem=wide_send.at[phase, c],
                recv_sem=wide_recv.at[phase, c],
                device_id={"wide": peer},
                device_id_type=pl.DeviceIdType.MESH,
            ).start()

        middle = n // 2
        one_copy(lax.rem(me + middle, n))

        def pair(k, carry):
            one_copy(lax.rem(me + middle + k, n))
            one_copy(lax.rem(me + middle - k, n))
            return carry

        lax.fori_loop(1, middle, pair, 0)

    def whole(ref, c, sem):
        view = ref.at[c, pl.ds(0, n - 1), pl.ds(0, cap)]
        return pltpu.make_async_copy(view, view, sem)

    for c in range(comps):
        going[c] = one_hot_dot(pick_mask[...], contributions[0, c]).reshape(n, capp, nodes)
        if c == 0:
            pl.semaphore_wait(barrier, n)
        exchange(going, coming, c, 0)
        coming[c, me] = going[c, me]

    sum_mask[...] = row_mask_of(arrival_row[...], sum_mask.shape)
    spread_mask[...] = mask_of(arrival_col[...], spread_mask.shape, 1)
    place_mask[...] = row_mask_of(send_row[...], place_mask.shape)

    mine = pl.multiple_of(side * half, half)
    theirs = pl.multiple_of((1 - side) * half, half)
    is_slave = side == 0

    for c in range(comps):
        whole(coming, c, wide_recv.at[0, c]).wait()
        sums[c] = one_hot_dot(sum_mask[...], coming[c].reshape(slots, nodes))
        swap = pltpu.make_async_remote_copy(
            src_ref=sums.at[c, pl.ds(theirs, half)],
            dst_ref=other_sums.at[c],
            send_sem=pair_send.at[0, c],
            recv_sem=pair_recv.at[0, c],
            device_id={"narrow": 1 - side},
            device_id_type=pl.DeviceIdType.MESH,
        )
        swap.start()
        if c == 0:
            for fetch in fetches:
                fetch.wait()
        swap.wait()

        def condense(g, carry):
            first = pl.multiple_of(g * GROUP, GROUP)
            rows = pl.ds(first, GROUP)
            own = sums[c, pl.ds(pl.multiple_of(mine + first, GROUP), GROUP), :]
            other = other_sums[c, rows, :]
            slave = jnp.where(is_slave, own, other)
            master = jnp.where(is_slave, other, own)
            scale = diagonal[pl.ds(pl.multiple_of(mine + first, GROUP), GROUP), :]
            low = (slave / scale).astype(jnp.bfloat16)
            condensed = master + block_products(low, lambda b: mortar[first + b], False)
            master_fix = block_products(
                condensed.astype(jnp.bfloat16), lambda b: inverse[first + b], True
            )
            slave_fix = (
                block_products(master_fix.astype(jnp.bfloat16), lambda b: mortar[first + b], True)
                / scale
            )
            fixes[c, pl.ds(pl.multiple_of(mine + first, GROUP), GROUP), :] = jnp.where(
                is_slave, slave_fix, master_fix
            )
            other_fix[c, rows, :] = jnp.where(is_slave, master_fix, slave_fix)
            return carry

        lax.fori_loop(0, half // GROUP, condense, 0)
        back = pltpu.make_async_remote_copy(
            src_ref=other_fix.at[c],
            dst_ref=fixes.at[c, pl.ds(mine, half)],
            send_sem=pair_send.at[1, c],
            recv_sem=pair_recv.at[1, c],
            device_id={"narrow": 1 - side},
            device_id_type=pl.DeviceIdType.MESH,
        )
        back.start()
        back.wait()
        returning[c] = one_hot_dot(spread_mask[...], fixes[c]).reshape(n, capp, nodes)
        exchange(returning, returned, c, 1)
        returned[c, me] = returning[c, me]

    for c in range(comps):
        whole(returned, c, wide_recv.at[1, c]).wait()
        out[0, c] = one_hot_dot(place_mask[...], returned[c].reshape(slots, nodes))
    for c in range(comps):
        whole(going, c, wide_send.at[0, c]).wait()
        whole(returning, c, wide_send.at[1, c]).wait()


def shards(contributions, send_map, arrival_map, dual_diagonal, mortar, master_inverse):
    n = lax.axis_size("wide")
    _, comps, row_count, nodes = contributions.shape
    blocks = dual_diagonal.shape[0]
    half = blocks // lax.axis_size("narrow")
    cap = send_map.shape[1] // n
    capp = -(-cap // SUBLANES) * SUBLANES
    slots = n * capp

    def padded(ids):
        return jnp.pad(
            ids.reshape(n, cap), ((0, 0), (0, capp - cap)), constant_values=-1
        )

    send = padded(send_map)
    arrival = padded(arrival_map)
    f32, bf16 = jnp.float32, jnp.bfloat16
    vmem = pl.BlockSpec(memory_space=pltpu.VMEM)
    hbm = pl.BlockSpec(memory_space=pl.ANY)
    travel = pltpu.VMEM((comps, n, capp, nodes), f32)
    return pl.pallas_call(
        functools.partial(kernel, n, cap),
        out_shape=jax.ShapeDtypeStruct((1, comps, row_count, nodes), f32),
        in_specs=[vmem] * 6 + [hbm] * 2,
        out_specs=vmem,
        scratch_shapes=[
            pltpu.VMEM((slots, row_count), bf16),
            pltpu.VMEM((blocks, slots), bf16),
            pltpu.VMEM((slots, blocks), bf16),
            pltpu.VMEM((row_count, slots), bf16),
            travel,
            travel,
            travel,
            travel,
            pltpu.VMEM((comps, blocks, nodes), f32),
            pltpu.VMEM((comps, half, nodes), f32),
            pltpu.VMEM((comps, half, nodes), f32),
            pltpu.VMEM((comps, blocks, nodes), f32),
            pltpu.VMEM((half, nodes, nodes), bf16),
            pltpu.VMEM((half, nodes, nodes), bf16),
            pltpu.SemaphoreType.DMA((2,)),
            pltpu.SemaphoreType.DMA((2, comps)),
            pltpu.SemaphoreType.DMA((2, comps)),
            pltpu.SemaphoreType.DMA((2, comps)),
            pltpu.SemaphoreType.DMA((2, comps)),
        ],
        compiler_params=pltpu.CompilerParams(
            collective_id=0, has_side_effects=True, vmem_limit_bytes=48 * 1024 * 1024
        ),
    )(
        contributions,
        send.reshape(slots, 1),
        jnp.broadcast_to(send.reshape(1, slots), (SUBLANES, slots)),
        arrival.reshape(slots, 1),
        jnp.broadcast_to(arrival.reshape(1, slots), (SUBLANES, slots)),
        dual_diagonal,
        mortar,
        master_inverse,
    )


def solution(mesh):
    placed = (
        P("narrow", None, "wide", None),
        P("wide", None),
        P("wide", None),
        P("wide", None),
        P("wide", None, None),
        P("wide", None, None),
    )
    return jax.shard_map(
        shards,
        mesh=mesh,
        in_specs=placed,
        out_specs=P("narrow", None, "wide", None),
        check_vma=False,
    )
```

```python
import functools

import jax
import jax.numpy as jnp
from jax import lax
from jax.experimental import pallas as pl
from jax.experimental.pallas import tpu as pltpu
from jax.sharding import PartitionSpec as P

GROUP = 16
SUBLANES = 8


def one_hot_dot(mask, values):
    high = values.astype(jnp.bfloat16)
    low = (values - high.astype(jnp.float32)).astype(jnp.bfloat16)
    return jnp.dot(mask, high, preferred_element_type=jnp.float32) + jnp.dot(
        mask, low, preferred_element_type=jnp.float32
    )


def block_products(vectors, matrices, transposed):
    rows = lax.broadcasted_iota(jnp.int32, vectors.shape, 0)
    total = jnp.zeros(vectors.shape, jnp.float32)
    for b in range(vectors.shape[0]):
        product = lax.dot_general(
            vectors,
            matrices(b),
            (((1,), (1 if transposed else 0,)), ((), ())),
            preferred_element_type=jnp.float32,
        )
        total = jnp.where(rows == b, product, total)
    return total


def kernel(
    n,
    cap,
    contributions,
    send_col,
    send_row,
    arrival_col,
    arrival_row,
    diagonal,
    mortar_hbm,
    inverse_hbm,
    out,
    pick_mask,
    sum_mask,
    spread_mask,
    place_mask,
    going,
    coming,
    returning,
    returned,
    sums,
    other_sums,
    other_fix,
    fixes,
    mortar,
    inverse,
    fetch_sem,
    wide_send,
    wide_recv,
    pair_send,
    pair_recv,
):
    me = lax.axis_index("wide")
    side = lax.axis_index("narrow")
    comps, row_count, nodes = out.shape[1:]
    capp = coming.shape[2]
    slots = n * capp
    half = mortar.shape[0]

    fetches = [
        pltpu.make_async_copy(mortar_hbm.at[pl.ds(side * half, half)], mortar, fetch_sem.at[0]),
        pltpu.make_async_copy(inverse_hbm.at[pl.ds(side * half, half)], inverse, fetch_sem.at[1]),
    ]

    if capp > cap:
        last = pl.ds(capp - SUBLANES, SUBLANES)
        empty = jnp.zeros((comps, n, SUBLANES, nodes), jnp.float32)
        coming[:, :, last, :] = empty
        returned[:, :, last, :] = empty

    barrier = pltpu.get_barrier_semaphore()

    def greet(k, carry):
        pl.semaphore_signal(barrier, inc=1, device_id={"wide": lax.rem(me + k, n)}, device_id_type=pl.DeviceIdType.MESH)
        return carry

    lax.fori_loop(1, n, greet, 0)
    pl.semaphore_signal(barrier, inc=1, device_id={"narrow": 1 - side}, device_id_type=pl.DeviceIdType.MESH)
    for fetch in fetches:
        fetch.start()


    def mask_of(ids, shape, axis):
        return jnp.where(ids == lax.broadcasted_iota(jnp.int32, shape, axis), 1.0, 0.0).astype(jnp.bfloat16)

    def row_mask_of(ids, shape):
        tiles = (shape[0] // SUBLANES, SUBLANES, shape[1])
        rows = lax.broadcasted_iota(jnp.int32, tiles, 0) * SUBLANES + lax.broadcasted_iota(
            jnp.int32, tiles, 1
        )
        return jnp.where(ids[None] == rows, 1.0, 0.0).reshape(shape).astype(jnp.bfloat16)

    pick_mask[...] = mask_of(send_col[...], pick_mask.shape, 1)

    def exchange(source, target, c, phase):
        def one_copy(peer):
            pltpu.make_async_remote_copy(
                src_ref=source.at[c, peer, pl.ds(0, cap)],
                dst_ref=target.at[c, me, pl.ds(0, cap)],
                send_sem=wide_send.at[phase, c],
                recv_sem=wide_recv.at[phase, c],
                device_id={"wide": peer},
                device_id_type=pl.DeviceIdType.MESH,
            ).start()

        middle = n // 2
        one_copy(lax.rem(me + middle, n))

        def pair(k, carry):
            one_copy(lax.rem(me + middle + k, n))
            one_copy(lax.rem(me + middle - k, n))
            return carry

        lax.fori_loop(1, middle, pair, 0)

    def whole(ref, c, sem):
        view = ref.at[c, pl.ds(0, n - 1), pl.ds(0, cap)]
        return pltpu.make_async_copy(view, view, sem)

    for c in range(comps):
        going[c] = one_hot_dot(pick_mask[...], contributions[0, c]).reshape(n, capp, nodes)
        if c == 0:
            pl.semaphore_wait(barrier, n)
        exchange(going, coming, c, 0)
        coming[c, me] = going[c, me]

    sum_mask[...] = row_mask_of(arrival_row[...], sum_mask.shape)
    spread_mask[...] = mask_of(arrival_col[...], spread_mask.shape, 1)
    place_mask[...] = row_mask_of(send_row[...], place_mask.shape)

    mine = pl.multiple_of(side * half, half)
    theirs = pl.multiple_of((1 - side) * half, half)
    is_slave = side == 0

    for c in range(comps):
        whole(coming, c, wide_recv.at[0, c]).wait()
        sums[c] = one_hot_dot(sum_mask[...], coming[c].reshape(slots, nodes))
        swap = pltpu.make_async_remote_copy(
            src_ref=sums.at[c, pl.ds(theirs, half)],
            dst_ref=other_sums.at[c],
            send_sem=pair_send.at[0, c],
            recv_sem=pair_recv.at[0, c],
            device_id={"narrow": 1 - side},
            device_id_type=pl.DeviceIdType.MESH,
        )
        swap.start()
        if c == 0:
            for fetch in fetches:
                fetch.wait()
        swap.wait()

        def condense(g, carry):
            first = pl.multiple_of(g * GROUP, GROUP)
            rows = pl.ds(first, GROUP)
            own = sums[c, pl.ds(pl.multiple_of(mine + first, GROUP), GROUP), :]
            other = other_sums[c, rows, :]
            slave = jnp.where(is_slave, own, other)
            master = jnp.where(is_slave, other, own)
            scale = diagonal[pl.ds(pl.multiple_of(mine + first, GROUP), GROUP), :]
            low = (slave / scale).astype(jnp.bfloat16)
            condensed = master + block_products(low, lambda b: mortar[first + b], False)
            master_fix = block_products(
                condensed.astype(jnp.bfloat16), lambda b: inverse[first + b], True
            )
            slave_fix = (
                block_products(master_fix.astype(jnp.bfloat16), lambda b: mortar[first + b], True)
                / scale
            )
            fixes[c, pl.ds(pl.multiple_of(mine + first, GROUP), GROUP), :] = jnp.where(
                is_slave, slave_fix, master_fix
            )
            other_fix[c, rows, :] = jnp.where(is_slave, master_fix, slave_fix)
            return carry

        lax.fori_loop(0, half // GROUP, condense, 0, unroll=2)
        back = pltpu.make_async_remote_copy(
            src_ref=other_fix.at[c],
            dst_ref=fixes.at[c, pl.ds(mine, half)],
            send_sem=pair_send.at[1, c],
            recv_sem=pair_recv.at[1, c],
            device_id={"narrow": 1 - side},
            device_id_type=pl.DeviceIdType.MESH,
        )
        back.start()
        back.wait()
        returning[c] = one_hot_dot(spread_mask[...], fixes[c]).reshape(n, capp, nodes)
        exchange(returning, returned, c, 1)
        returned[c, me] = returning[c, me]

    for c in range(comps):
        whole(returned, c, wide_recv.at[1, c]).wait()
        out[0, c] = one_hot_dot(place_mask[...], returned[c].reshape(slots, nodes))
    for c in range(comps):
        whole(going, c, wide_send.at[0, c]).wait()
        whole(returning, c, wide_send.at[1, c]).wait()


def shards(contributions, send_map, arrival_map, dual_diagonal, mortar, master_inverse):
    n = lax.axis_size("wide")
    _, comps, row_count, nodes = contributions.shape
    blocks = dual_diagonal.shape[0]
    half = blocks // lax.axis_size("narrow")
    cap = send_map.shape[1] // n
    capp = -(-cap // SUBLANES) * SUBLANES
    slots = n * capp

    def padded(ids):
        return jnp.pad(
            ids.reshape(n, cap), ((0, 0), (0, capp - cap)), constant_values=-1
        )

    send = padded(send_map)
    arrival = padded(arrival_map)
    f32, bf16 = jnp.float32, jnp.bfloat16
    vmem = pl.BlockSpec(memory_space=pltpu.VMEM)
    hbm = pl.BlockSpec(memory_space=pl.ANY)
    travel = pltpu.VMEM((comps, n, capp, nodes), f32)
    return pl.pallas_call(
        functools.partial(kernel, n, cap),
        out_shape=jax.ShapeDtypeStruct((1, comps, row_count, nodes), f32),
        in_specs=[vmem] * 6 + [hbm] * 2,
        out_specs=vmem,
        scratch_shapes=[
            pltpu.VMEM((slots, row_count), bf16),
            pltpu.VMEM((blocks, slots), bf16),
            pltpu.VMEM((slots, blocks), bf16),
            pltpu.VMEM((row_count, slots), bf16),
            travel,
            travel,
            travel,
            travel,
            pltpu.VMEM((comps, blocks, nodes), f32),
            pltpu.VMEM((comps, half, nodes), f32),
            pltpu.VMEM((comps, half, nodes), f32),
            pltpu.VMEM((comps, blocks, nodes), f32),
            pltpu.VMEM((half, nodes, nodes), bf16),
            pltpu.VMEM((half, nodes, nodes), bf16),
            pltpu.SemaphoreType.DMA((2,)),
            pltpu.SemaphoreType.DMA((2, comps)),
            pltpu.SemaphoreType.DMA((2, comps)),
            pltpu.SemaphoreType.DMA((2, comps)),
            pltpu.SemaphoreType.DMA((2, comps)),
        ],
        compiler_params=pltpu.CompilerParams(
            collective_id=0, has_side_effects=True, vmem_limit_bytes=48 * 1024 * 1024
        ),
    )(
        contributions,
        send.reshape(slots, 1),
        jnp.broadcast_to(send.reshape(1, slots), (SUBLANES, slots)),
        arrival.reshape(slots, 1),
        jnp.broadcast_to(arrival.reshape(1, slots), (SUBLANES, slots)),
        dual_diagonal,
        mortar,
        master_inverse,
    )


def solution(mesh):
    placed = (
        P("narrow", None, "wide", None),
        P("wide", None),
        P("wide", None),
        P("wide", None),
        P("wide", None, None),
        P("wide", None, None),
    )
    return jax.shard_map(
        shards,
        mesh=mesh,
        in_specs=placed,
        out_specs=P("narrow", None, "wide", None),
        check_vma=False,
    )
```
